32 devices in a mesh: py: 4 (over y, core), pz: 8 (over z, x).
Axes of the slice: x: 2, y: 2, z: 4, core: 2. Of those that a mesh axis runs over, the one named last changes fastest.
Arguments:
- wavefunctions: float32 [2, 8, 128, 128, 128], P(None, None, 'pz', 'py'), may hold values from -6 to 6
- potential: float32 [128, 128, 128], P('pz', 'py'), may hold values from -4 to 4
- cutoff_sq: int32 [1], replicated, may hold values from 2304 to 4096
- locked_mask: int32 [8], replicated, may hold values 0 or 1
Outputs:
- applied: float32 [2, 8, 128, 128, 128], P(None, None, 'pz', 'py')
- rayleigh: float32 [8], replicated
- residual_norm: float32 [8], replicated
The draws below stay inside these ranges and needn't reach their ends.
All inputs are finite; a program needn't handle non-finite values.
Results may differ from the reference program's by a relative error of at most 0.00005.
Values sent between devices are 32-bit elements; how exact they have to be, the bound alone decides.
A program may use at most 64 MiB of HBM per device.

```python
import math
import jax
import jax.numpy as jnp
from jax import lax

GRID = 128
NB = 8


def place_ends(entries, own_key, least, largest):
    extent = entries.shape
    place = [jax.random.randint(jax.random.fold_in(own_key, axis), (), 0, extent[axis]) for axis in range(len(extent))]
    entries = entries.at[tuple(place)].set(least)
    longest = extent.index(max(extent))
    place[longest] = (place[longest] + 1) % extent[longest]
    return entries.at[tuple(place)].set(largest)


def steps_of(stream_key, dims, pieces, smallest, top_value):
    def one(dim, parts):
        draws = jax.random.uniform(jax.random.fold_in(jax.random.fold_in(stream_key, 6), dim), (parts,), jnp.float32, smallest / len(pieces), top_value / len(pieces))
        return jnp.repeat(jnp.exp(draws), dims[dim] // parts).reshape((-1,) + (1,) * (len(dims) - dim - 1))

    level = one(*pieces[0])
    for cut in pieces[1:]:
        level = level * one(*cut)
    return level


def centred(rng, extent, scale, limit, shards=(), held_as=jnp.bfloat16):
    result = jax.random.normal(rng, extent, jnp.float32) * scale
    if len(shards) > 0:
        result = steps_of(rng, extent, shards, -0.22, 0.18) * result
    return jnp.clip(result, min=-limit, max=limit).astype(held_as)


def setup_inputs(seed: int = 0) -> dict:
    keys = jax.random.split(jax.random.key(seed), 5)
    return {
        "wavefunctions": centred(keys[0], (2, NB, GRID, GRID, GRID), 1.0, 6.0, ((2, 8), (3, 4)), jnp.float32),
        "potential": centred(keys[1], (GRID, GRID, GRID), 1.0, 4.0, ((0, 8), (1, 4)), jnp.float32),
        "cutoff_sq": jax.random.randint(keys[2], (1,), GRID * GRID * 9 // 64, GRID * GRID // 4 + 1).astype(jnp.int32),
        "locked_mask": place_ends((jax.random.randint(keys[3], (NB,), 0, 4) < 1).astype(jnp.int32), jax.random.fold_in(keys[3], 1), 0, 1),
    }


def reference(wavefunctions, potential, cutoff_sq, locked_mask):
    freq = jnp.arange(GRID, dtype=jnp.int32)
    signed = jnp.where(freq < GRID // 2, freq, freq - GRID)
    square = signed * signed
    total = square[:, None, None] + square[None, :, None] + square[None, None, :]
    keep = (total <= cutoff_sq[0]).astype(jnp.float32)
    kinetic = 0.5 * (math.pi / GRID) ** 2 * total.astype(jnp.float32) * keep

    def one_band(pair):
        real_part, imag_part = pair
        field = real_part + 1j * imag_part
        spectrum = jnp.fft.fftn(field)
        back = jnp.fft.ifftn(spectrum * kinetic)
        return (jnp.real(back) + potential * real_part, jnp.imag(back) + potential * imag_part)
    applied_real, applied_imag = lax.map(one_band, (wavefunctions[0], wavefunctions[1]))
    applied = jnp.stack([applied_real, applied_imag])
    norm_sq = lax.optimization_barrier(jnp.sum(wavefunctions * wavefunctions, axis=(0, 2, 3, 4)))
    correlation = lax.optimization_barrier(jnp.sum(wavefunctions * applied, axis=(0, 2, 3, 4)))
    rayleigh = correlation / norm_sq
    residual = applied - rayleigh[None, :, None, None, None] * wavefunctions
    residual_sq = lax.optimization_barrier(jnp.sum(residual * residual, axis=(0, 2, 3, 4)))
    residual_norm = jnp.sqrt(residual_sq / norm_sq) * (1.0 - locked_mask.astype(jnp.float32))
    return (applied, rayleigh, residual_norm)
```

```python
import math

import jax
import jax.numpy as jnp
from jax import lax
from jax.sharding import PartitionSpec as P

PREC = lax.Precision.HIGH


def make_tables(length, inverse):
    counter = jnp.arange(length, dtype=jnp.int32)
    phase = counter[:, None] * counter[None, :] % length
    angle = 2.0 * math.pi / length * phase.astype(jnp.float32)
    if inverse:
        return (jnp.cos(angle) / length, jnp.sin(angle) / length)
    return (jnp.cos(angle), -jnp.sin(angle))


def transform(form, pair, tables):
    re, im = pair
    cosines, sines = tables

    def dot(field, table):
        return jnp.einsum(form, field, table, precision=PREC)

    return (dot(re, cosines) - dot(im, sines), dot(re, sines) + dot(im, cosines))


def exchange(pair, axis, split, concat):
    return tuple(
        lax.all_to_all(part, axis, split_axis=split, concat_axis=concat, tiled=True)
        for part in pair
    )


def signed_square(counter, length):
    signed = jnp.where(counter < length // 2, counter, counter - length)
    return signed * signed


def body(wavefunctions, potential, cutoff_sq, locked_mask):
    length = wavefunctions.shape[4]
    forward = make_tables(length, False)
    inverse = make_tables(length, True)
    along_x = "bzyn,kn->bzyk"
    along_y = "bznx,kn->bzkx"
    along_z = "bnyx,kn->bkyx"
    pair = (wavefunctions[0], wavefunctions[1])
    pair = transform(along_x, pair, forward)
    pair = exchange(pair, "py", 0, 2)
    pair = transform(along_y, pair, forward)
    pair = exchange(pair, "pz", 2, 1)
    pair = transform(along_z, pair, forward)
    rows = pair[0].shape[2]
    full_sq = signed_square(jnp.arange(length, dtype=jnp.int32), length)
    own = lax.axis_index("pz") * rows + jnp.arange(rows, dtype=jnp.int32)
    own_sq = signed_square(own, length)
    total = full_sq[:, None, None] + own_sq[None, :, None] + full_sq[None, None, :]
    keep = (total <= cutoff_sq[0]).astype(jnp.float32)
    kinetic = 0.5 * (math.pi / length) ** 2 * total.astype(jnp.float32) * keep
    pair = tuple(part * kinetic[None] for part in pair)
    pair = transform(along_z, pair, inverse)
    pair = exchange(pair, "pz", 1, 2)
    pair = transform(along_y, pair, inverse)
    pair = exchange(pair, "py", 2, 0)
    pair = transform(along_x, pair, inverse)
    applied = jnp.stack(pair) + potential[None, None] * wavefunctions
    norm_own = jnp.sum(wavefunctions * wavefunctions, axis=(0, 2, 3, 4))
    corr_own = jnp.sum(wavefunctions * applied, axis=(0, 2, 3, 4))
    shift = jnp.where(norm_own > 0.0, corr_own / jnp.where(norm_own > 0.0, norm_own, 1.0), 0.0)
    rest = applied - shift[None, :, None, None, None] * wavefunctions
    rest_sq = jnp.sum(rest * rest, axis=(0, 2, 3, 4))
    rest_dot = jnp.sum(rest * wavefunctions, axis=(0, 2, 3, 4))
    sums = jnp.stack([norm_own, corr_own, shift, rest_sq, rest_dot])
    every = lax.all_gather(sums, ("py", "pz"))
    norm_all, corr_all, shift_all, sq_all, dot_all = (every[:, i] for i in range(5))
    norm_sq = jnp.sum(norm_all, axis=0)
    rayleigh = jnp.sum(corr_all, axis=0) / norm_sq
    gap = shift_all - rayleigh[None]
    residual_sq = jnp.sum(sq_all + 2.0 * gap * dot_all + gap * gap * norm_all, axis=0)
    residual_sq = jnp.maximum(residual_sq, 0.0)
    residual_norm = jnp.sqrt(residual_sq / norm_sq) * (1.0 - locked_mask.astype(jnp.float32))
    return (applied, rayleigh, residual_norm)


def solution(mesh):
    in_specs = (P(None, None, "pz", "py", None), P("pz", "py", None), P(), P())
    out_specs = (P(None, None, "pz", "py", None), P(), P())
    return jax.shard_map(body, mesh=mesh, in_specs=in_specs, out_specs=out_specs, check_vma=False)
```

```python
import functools
import math

import jax
import jax.numpy as jnp
from jax import lax
from jax.experimental import pallas as pl
from jax.experimental.pallas import tpu as pltpu
from jax.sharding import PartitionSpec as P

PREC = lax.Precision.HIGHEST
MESH = pl.DeviceIdType.MESH


def make_tables(length, inverse):
    counter = jnp.arange(length, dtype=jnp.int32)
    phase = counter[:, None] * counter[None, :] % length
    angle = 2.0 * math.pi / length * phase.astype(jnp.float32)
    if inverse:
        return (jnp.cos(angle) / length, jnp.sin(angle) / length)
    return (jnp.cos(angle), -jnp.sin(angle))


def transform(form, pair, tables):
    re, im = pair
    cosines, sines = tables

    def dot(field, table):
        return jnp.einsum(form, field, table, precision=PREC)

    return (dot(re, cosines) - dot(im, sines), dot(re, sines) + dot(im, cosines))


def exchange(pair, axis, split, concat):
    return tuple(
        lax.all_to_all(part, axis, split_axis=split, concat_axis=concat, tiled=True)
        for part in pair
    )


def signed_square(counter, length):
    signed = jnp.where(counter < length // 2, counter, counter - length)
    return signed * signed


def right_matrix(tables):
    cosines, sines = tables
    top = jnp.concatenate([cosines, sines], axis=1)
    return jnp.concatenate([top, jnp.concatenate([-sines, cosines], axis=1)], axis=0)


def dot(left, right):
    return jnp.dot(left, right, precision=PREC, preferred_element_type=jnp.float32)


def main_kernel(
    size_y, size_z, chunks,
    u_ref, kin_ref, xf_ref, xi_ref, lf_ref, li_ref, out_ref,
    a1, r1, a2, r2, r3,
    s1, q1, s2, q2, s3, q3, s4, q4,
):
    me_y, me_z = lax.axis_index("py"), lax.axis_index("pz")
    _, bands, rows_z, rows_y, length = u_ref.shape
    slots = bands // size_y
    rows_k = length // size_z
    step = rows_z // chunks
    high = length

    barrier = pltpu.get_barrier_semaphore()
    for d in range(1, size_y):
        pl.semaphore_signal(barrier, inc=1, device_id={"py": (me_y + d) % size_y}, device_id_type=MESH)
    for d in range(1, size_z):
        pl.semaphore_signal(barrier, inc=1, device_id={"pz": (me_z + d) % size_z}, device_id_type=MESH)
    pl.semaphore_wait(barrier, size_y + size_z - 2)

    def copy1(s, c, d):
        to = (me_y + d) % size_y
        return pltpu.make_async_remote_copy(
            src_ref=a1.at[:, to * slots + s, pl.ds(c * step, step)],
            dst_ref=r1.at[:, s, pl.ds(c * step, step), me_y],
            send_sem=s1.at[s, c, d - 1], recv_sem=q1.at[s, c, d - 1],
            device_id={"py": to}, device_id_type=MESH)

    def copy2(s, c, d):
        to = (me_z + d) % size_z
        rows = step * rows_k
        return pltpu.make_async_remote_copy(
            src_ref=a2.at[:, s, to, pl.ds(pl.multiple_of(c * rows, rows), rows)],
            dst_ref=r2.at[:, s, pl.ds(pl.multiple_of((me_z * chunks + c) * rows, rows), rows)],
            send_sem=s2.at[s, c, d - 1], recv_sem=q2.at[s, c, d - 1],
            device_id={"pz": to}, device_id_type=MESH)

    def copy3(s, c, d):
        to = (me_z + d) % size_z
        rows = step * rows_k
        return pltpu.make_async_remote_copy(
            src_ref=r2.at[:, s, pl.ds(pl.multiple_of((to * chunks + c) * rows, rows), rows)],
            dst_ref=r3.at[:, s, me_z, pl.ds(pl.multiple_of(c * rows, rows), rows)],
            send_sem=s3.at[s, c, d - 1], recv_sem=q3.at[s, c, d - 1],
            device_id={"pz": to}, device_id_type=MESH)

    def copy4(s, c, d):
        to = (me_y + d) % size_y
        return pltpu.make_async_remote_copy(
            src_ref=r1.at[:, s, pl.ds(c * step, step), to],
            dst_ref=out_ref.at[:, me_y * slots + s, pl.ds(c * step, step)],
            send_sem=s4.at[s, c, d - 1], recv_sem=q4.at[s, c, d - 1],
            device_id={"py": to}, device_id_type=MESH)

    order_z = sorted(range(1, size_z), key=lambda d: -min(d, size_z - d))

    for s in range(slots):
        def forward_x(c, carry):
            for d in list(range(1, size_y)) + [0]:
                band = (me_y + d) % size_y * slots + s
                zs = pl.ds(c * step, step)
                rows = jnp.concatenate(
                    [u_ref[p, band, zs].reshape(step * rows_y, length) for p in range(2)], axis=1)
                done = dot(rows, xf_ref[...])
                for p in range(2):
                    part = done[:, p * high : (p + 1) * high].reshape(step, rows_y, length)
                    if d == 0:
                        r1[p, s, zs, me_y] = part
                    else:
                        a1[p, band, zs] = part
                if d > 0:
                    copy1(s, c, d).start()
            return carry
        lax.fori_loop(0, chunks, forward_x, 0)

    for s in range(slots):
        def forward_y(c, carry):
            for d in range(1, size_y):
                copy1(s, c, d).wait_recv()
            for i in range(0, step, 2):
                sides = []
                for z in (c * step + i, c * step + i + 1):
                    sides.append(jnp.concatenate(
                        [r1[p, s, z].reshape(length, length) for p in range(2)], axis=0))
                done = dot(lf_ref[...], jnp.concatenate(sides, axis=1))
                for p in range(2):
                    for e in range(2):
                        at = pl.ds(pl.multiple_of((c * step + i + e) * rows_k, rows_k), rows_k)
                        part = done[p * high : (p + 1) * high, e * high : (e + 1) * high]
                        a2[p, s, :, at] = part.reshape(size_z, rows_k, length)
            for d in order_z:
                copy2(s, c, d).start()
            rows = step * rows_k
            own = pl.ds(pl.multiple_of(c * rows, rows), rows)
            r2[:, s, pl.ds(pl.multiple_of((me_z * chunks + c) * rows, rows), rows)] = a2[:, s, me_z, own]
            return carry
        lax.fori_loop(0, chunks, forward_y, 0)

    for s in range(slots):
        def arrive2(c, carry):
            for d in range(1, size_z):
                copy2(s, c, d).wait_recv()
            return carry
        lax.fori_loop(0, chunks, arrive2, 0)

        def both_z(h, carry):
            sides = []
            for k in (2 * h, 2 * h + 1):
                sides.append(jnp.concatenate(
                    [r2[p, s, pl.ds(k, length, stride=rows_k)] for p in range(2)], axis=0))
            spectrum = dot(lf_ref[...], jnp.concatenate(sides, axis=1))
            weight = jnp.concatenate([kin_ref[2 * h], kin_ref[2 * h + 1]], axis=1)
            weight = jnp.concatenate([weight, weight], axis=0)
            done = dot(li_ref[...], spectrum * weight)
            for p in range(2):
                for e in range(2):
                    r2[p, s, pl.ds(2 * h + e, length, stride=rows_k)] = done[
                        p * high : (p + 1) * high, e * high : (e + 1) * high]
            return carry
        lax.fori_loop(0, rows_k // 2, both_z, 0)

        def leave3(c, carry):
            for d in order_z:
                copy3(s, c, d).start()
            return carry
        lax.fori_loop(0, chunks, leave3, 0)
        every = rows_z * rows_k
        r3[:, s, me_z] = r2[:, s, pl.ds(pl.multiple_of(me_z * every, every), every)]

    for s in range(slots):
        def inverse_y(c, carry):
            for d in range(1, size_z):
                copy3(s, c, d).wait_recv()
            for i in range(0, step, 2):
                sides = []
                for e in range(2):
                    at = pl.ds(pl.multiple_of((c * step + i + e) * rows_k, rows_k), rows_k)
                    sides.append(jnp.concatenate(
                        [r3[p, s, :, at].reshape(length, length) for p in range(2)], axis=0))
                done = dot(li_ref[...], jnp.concatenate(sides, axis=1))
                for p in range(2):
                    for e in range(2):
                        part = done[p * high : (p + 1) * high, e * high : (e + 1) * high]
                        r1[p, s, c * step + i + e] = part.reshape(size_y, rows_y, length)
            for d in range(1, size_y):
                copy4(s, c, d).start()
            zs = pl.ds(c * step, step)
            out_ref[:, me_y * slots + s, zs] = r1[:, s, zs, me_y]
            return carry
        lax.fori_loop(0, chunks, inverse_y, 0)

    for s in range(slots):
        def inverse_x(c, carry):
            zs = pl.ds(c * step, step)
            for d in range(size_y):
                band = (me_y + size_y - d) % size_y * slots + s
                if d > 0:
                    copy4(s, c, d).wait_recv()
                rows = jnp.concatenate(
                    [out_ref[p, band, zs].reshape(step * rows_y, length) for p in range(2)], axis=1)
                done = dot(rows, xi_ref[...])
                for p in range(2):
                    out_ref[p, band, zs] = done[:, p * high : (p + 1) * high].reshape(
                        step, rows_y, length)
            return carry
        lax.fori_loop(0, chunks, inverse_x, 0)

    for s in range(slots):
        def settle(c, carry):
            for d in range(1, size_y):
                copy1(s, c, d).wait_send()
                copy4(s, c, d).wait_send()
            for d in range(1, size_z):
                copy2(s, c, d).wait_send()
                copy3(s, c, d).wait_send()
            return carry
        lax.fori_loop(0, chunks, settle, 0)


def fused_kinetic(wavefunctions, kinetic, forward, inverse):
    _, bands, rows_z, rows_y, length = wavefunctions.shape
    size_y, size_z = lax.axis_size("py"), lax.axis_size("pz")
    slots = bands // size_y
    rows_k = length // size_z
    chunks = rows_z // 4
    xf, xi = right_matrix(forward), right_matrix(inverse)
    vmem = pl.BlockSpec(memory_space=pltpu.VMEM)
    near = pltpu.SemaphoreType.DMA((slots, chunks, size_y - 1))
    far = pltpu.SemaphoreType.DMA((slots, chunks, size_z - 1))
    return pl.pallas_call(
        functools.partial(main_kernel, size_y, size_z, chunks),
        out_shape=jax.ShapeDtypeStruct(wavefunctions.shape, jnp.float32),
        in_specs=[vmem] * 6,
        out_specs=vmem,
        scratch_shapes=[
            pltpu.VMEM((2, bands, rows_z, rows_y, length), jnp.float32),
            pltpu.VMEM((2, slots, rows_z, size_y, rows_y, length), jnp.float32),
            pltpu.VMEM((2, slots, size_z, rows_z * rows_k, length), jnp.float32),
            pltpu.VMEM((2, slots, length * rows_k, length), jnp.float32),
            pltpu.VMEM((2, slots, size_z, rows_z * rows_k, length), jnp.float32),
            near, near, far, far, far, far, near, near,
        ],
        compiler_params=pltpu.CompilerParams(
            collective_id=0, has_side_effects=True, vmem_limit_bytes=67043328),
    )(wavefunctions, kinetic, xf, xi, xf.T, xi.T)


def gather_kernel(size_y, size_z, own_ref, out_ref, send, recv):
    me_y, me_z = lax.axis_index("py"), lax.axis_index("pz")
    me = me_y * size_z + me_z
    count = size_y * size_z
    barrier = pltpu.get_barrier_semaphore()

    def target(t):
        to = (me + t) % count
        return {"py": to // size_z, "pz": to % size_z}

    def greet(t, carry):
        pl.semaphore_signal(barrier, inc=1, device_id=target(t), device_id_type=MESH)
        return carry
    lax.fori_loop(1, count, greet, 0)
    pl.semaphore_wait(barrier, count - 1)

    def copy(t):
        return pltpu.make_async_remote_copy(
            src_ref=own_ref, dst_ref=out_ref.at[me], send_sem=send.at[t], recv_sem=recv.at[t],
            device_id=target(t), device_id_type=MESH)

    def leave(t, carry):
        copy(t).start()
        return carry
    lax.fori_loop(1, count, leave, 0)
    out_ref[me] = own_ref[...]

    def arrive(t, carry):
        copy(t).wait()
        return carry
    lax.fori_loop(1, count, arrive, 0)


def gather_sums(sums):
    size_y, size_z = lax.axis_size("py"), lax.axis_size("pz")
    count = size_y * size_z
    kinds, bands = sums.shape
    if count > 64:
        return lax.all_gather(sums, ("py", "pz"))
    own = jnp.pad(sums, ((0, 8 - kinds), (0, 128 - bands)))
    vmem = pl.BlockSpec(memory_space=pltpu.VMEM)
    every = pl.pallas_call(
        functools.partial(gather_kernel, size_y, size_z),
        out_shape=jax.ShapeDtypeStruct((count, 8, 128), jnp.float32),
        in_specs=[vmem],
        out_specs=vmem,
        scratch_shapes=[pltpu.SemaphoreType.DMA((count,)), pltpu.SemaphoreType.DMA((count,))],
        compiler_params=pltpu.CompilerParams(collective_id=1, has_side_effects=True),
    )(own)
    return every[:, :kinds, :bands]


def plain_kinetic(wavefunctions, kinetic, forward, inverse):
    along_x = "bzyn,kn->bzyk"
    along_y = "bznx,kn->bzkx"
    along_z = "bnyx,kn->bkyx"
    pair = (wavefunctions[0], wavefunctions[1])
    pair = transform(along_x, pair, forward)
    pair = exchange(pair, "py", 0, 2)
    pair = transform(along_y, pair, forward)
    pair = exchange(pair, "pz", 2, 1)
    pair = transform(along_z, pair, forward)
    pair = tuple(part * jnp.swapaxes(kinetic, 0, 1)[None] for part in pair)
    pair = transform(along_z, pair, inverse)
    pair = exchange(pair, "pz", 1, 2)
    pair = transform(along_y, pair, inverse)
    pair = exchange(pair, "py", 2, 0)
    pair = transform(along_x, pair, inverse)
    return jnp.stack(pair)


def body(wavefunctions, potential, cutoff_sq, locked_mask):
    length = wavefunctions.shape[4]
    forward = make_tables(length, False)
    inverse = make_tables(length, True)
    size_y, size_z = lax.axis_size("py"), lax.axis_size("pz")
    rows = length // size_z
    full_sq = signed_square(jnp.arange(length, dtype=jnp.int32), length)
    own = lax.axis_index("pz") * rows + jnp.arange(rows, dtype=jnp.int32)
    own_sq = signed_square(own, length)
    total = own_sq[:, None, None] + full_sq[None, :, None] + full_sq[None, None, :]
    keep = (total <= cutoff_sq[0]).astype(jnp.float32)
    kinetic = 0.5 * (math.pi / length) ** 2 * total.astype(jnp.float32) * keep
    fits = rows % 8 == 0 and wavefunctions.shape[2] % 4 == 0 and wavefunctions.shape[1] % size_y == 0
    if fits:
        back = fused_kinetic(wavefunctions, kinetic, forward, inverse)
    else:
        back = plain_kinetic(wavefunctions, kinetic, forward, inverse)
    applied = back + potential[None, None] * wavefunctions
    norm_own = jnp.sum(wavefunctions * wavefunctions, axis=(0, 2, 3, 4))
    corr_own = jnp.sum(wavefunctions * applied, axis=(0, 2, 3, 4))
    shift = jnp.where(norm_own > 0.0, corr_own / jnp.where(norm_own > 0.0, norm_own, 1.0), 0.0)
    rest = applied - shift[None, :, None, None, None] * wavefunctions
    rest_sq = jnp.sum(rest * rest, axis=(0, 2, 3, 4))
    rest_dot = jnp.sum(rest * wavefunctions, axis=(0, 2, 3, 4))
    sums = jnp.stack([norm_own, corr_own, shift, rest_sq, rest_dot])
    every = gather_sums(sums)
    norm_all, corr_all, shift_all, sq_all, dot_all = (every[:, i] for i in range(5))
    norm_sq = jnp.sum(norm_all, axis=0)
    rayleigh = jnp.sum(corr_all, axis=0) / norm_sq
    gap = shift_all - rayleigh[None]
    residual_sq = jnp.sum(sq_all + 2.0 * gap * dot_all + gap * gap * norm_all, axis=0)
    residual_sq = jnp.maximum(residual_sq, 0.0)
    residual_norm = jnp.sqrt(residual_sq / norm_sq) * (1.0 - locked_mask.astype(jnp.float32))
    return (applied, rayleigh, residual_norm)


def solution(mesh):
    in_specs = (P(None, None, "pz", "py", None), P("pz", "py", None), P(), P())
    out_specs = (P(None, None, "pz", "py", None), P(), P())
    return jax.shard_map(body, mesh=mesh, in_specs=in_specs, out_specs=out_specs, check_vma=False)
```

```python
import functools
import math

import jax
import jax.numpy as jnp
import numpy as np
from jax import lax
from jax.experimental import pallas as pl
from jax.experimental.pallas import tpu as pltpu
from jax.sharding import PartitionSpec as P

PREC = lax.Precision.HIGHEST
MESH = pl.DeviceIdType.MESH


def make_tables(length, inverse):
    counter = jnp.arange(length, dtype=jnp.int32)
    phase = counter[:, None] * counter[None, :] % length
    angle = 2.0 * math.pi / length * phase.astype(jnp.float32)
    if inverse:
        return (jnp.cos(angle) / length, jnp.sin(angle) / length)
    return (jnp.cos(angle), -jnp.sin(angle))


def transform(form, pair, tables):
    re, im = pair
    cosines, sines = tables

    def dot(field, table):
        return jnp.einsum(form, field, table, precision=PREC)

    return (dot(re, cosines) - dot(im, sines), dot(re, sines) + dot(im, cosines))


def exchange(pair, axis, split, concat):
    return tuple(
        lax.all_to_all(part, axis, split_axis=split, concat_axis=concat, tiled=True)
        for part in pair
    )


def signed_square(counter, length):
    signed = jnp.where(counter < length // 2, counter, counter - length)
    return signed * signed


def right_matrix(tables):
    cosines, sines = tables
    top = jnp.concatenate([cosines, sines], axis=1)
    return jnp.concatenate([top, jnp.concatenate([-sines, cosines], axis=1)], axis=0)


def fold_rows(length, extra):
    half = length // 2
    reach = {f: math.isqrt(half * half - f * f) for f in range(-half, half)}
    guests = [f for f in sorted(reach, key=lambda f: (reach[f], f)) if f != -half][:extra]
    free = [f for f in reach if f not in guests and f != -half]
    hosts = []
    for g in reversed(guests):
        fits = [f for f in free if reach[f] + reach[g] < half]
        if not fits:
            return None
        hosts.append(min(fits, key=lambda f: (abs(f), f)))
        free.remove(hosts[-1])
    hosts = hosts[::-1]
    plain = [f for f in sorted(reach) if f not in hosts and f not in guests]
    order = np.array(plain + hosts + guests)
    lanes = np.arange(length)
    signed = np.where(lanes < half, lanes, lanes - length)
    moved = np.roll(signed, half)
    mask = np.abs(signed)[None, :] <= np.array([reach[f] for f in hosts])[:, None]
    hosts, guests = np.array(hosts), np.array(guests)
    square = np.concatenate([
        np.array(plain)[:, None] ** 2 + signed[None, :] ** 2,
        np.where(mask, hosts[:, None] ** 2 + signed[None, :] ** 2,
                 guests[:, None] ** 2 + moved[None, :] ** 2)])
    return order % length, mask.astype(np.float32), square.astype(np.int32)


def dot(left, right):
    return jnp.dot(left, right, precision=PREC, preferred_element_type=jnp.float32)


def main_kernel(
    size_y, size_z, chunks,
    u_ref, kin_ref, xf_ref, xi_ref, lf_ref, li_ref, yf_ref, yi_ref, mask_ref, out_ref,
    a1, r1, a2, r2, r3,
    s1, q1, s2, q2, s3, q3, s4, q4,
):
    me_y, me_z = lax.axis_index("py"), lax.axis_index("pz")
    _, bands, rows_z, rows_y, length = u_ref.shape
    slots = bands // size_y
    rows_k = kin_ref.shape[0]
    extra = mask_ref.shape[0]
    hosts = length - 2 * extra
    step = rows_z // chunks
    high = length

    barrier = pltpu.get_barrier_semaphore()
    for d in range(1, size_y):
        pl.semaphore_signal(barrier, inc=1, device_id={"py": (me_y + d) % size_y}, device_id_type=MESH)
    for d in range(1, size_z):
        pl.semaphore_signal(barrier, inc=1, device_id={"pz": (me_z + d) % size_z}, device_id_type=MESH)
    pl.semaphore_wait(barrier, size_y + size_z - 2)

    def copy1(s, c, d):
        to = (me_y + d) % size_y
        return pltpu.make_async_remote_copy(
            src_ref=a1.at[:, to * slots + s, pl.ds(c * step, step)],
            dst_ref=r1.at[:, s, pl.ds(c * step, step), me_y],
            send_sem=s1.at[s, c, d - 1], recv_sem=q1.at[s, c, d - 1],
            device_id={"py": to}, device_id_type=MESH)

    def copy2(s, c, d):
        to = (me_z + d) % size_z
        rows = step * rows_k
        return pltpu.make_async_remote_copy(
            src_ref=a2.at[:, s, to, pl.ds(pl.multiple_of(c * rows, rows), rows)],
            dst_ref=r2.at[:, s, pl.ds(pl.multiple_of((me_z * chunks + c) * rows, rows), rows)],
            send_sem=s2.at[s, c, d - 1], recv_sem=q2.at[s, c, d - 1],
            device_id={"pz": to}, device_id_type=MESH)

    def copy3(s, c, d):
        to = (me_z + d) % size_z
        rows = step * rows_k
        return pltpu.make_async_remote_copy(
            src_ref=r2.at[:, s, pl.ds(pl.multiple_of((to * chunks + c) * rows, rows), rows)],
            dst_ref=r3.at[:, s, me_z, pl.ds(pl.multiple_of(c * rows, rows), rows)],
            send_sem=s3.at[s, c, d - 1], recv_sem=q3.at[s, c, d - 1],
            device_id={"pz": to}, device_id_type=MESH)

    def copy4(s, c, d):
        to = (me_y + d) % size_y
        return pltpu.make_async_remote_copy(
            src_ref=r1.at[:, s, pl.ds(c * step, step), to],
            dst_ref=out_ref.at[:, me_y * slots + s, pl.ds(c * step, step)],
            send_sem=s4.at[s, c, d - 1], recv_sem=q4.at[s, c, d - 1],
            device_id={"py": to}, device_id_type=MESH)

    order_z = sorted(range(1, size_z), key=lambda d: -min(d, size_z - d))

    for s in range(slots):
        def forward_x(c, carry):
            for d in list(range(1, size_y)) + [0]:
                band = (me_y + d) % size_y * slots + s
                zs = pl.ds(c * step, step)
                rows = jnp.concatenate(
                    [u_ref[p, band, zs].reshape(step * rows_y, length) for p in range(2)], axis=1)
                done = dot(rows, xf_ref[...])
                for p in range(2):
                    part = done[:, p * high : (p + 1) * high].reshape(step, rows_y, length)
                    if d == 0:
                        r1[p, s, zs, me_y] = part
                    else:
                        a1[p, band, zs] = part
                if d > 0:
                    copy1(s, c, d).start()
            return carry
        lax.fori_loop(0, chunks, forward_x, 0)

    for s in range(slots):
        def forward_y(c, carry):
            for d in range(1, size_y):
                copy1(s, c, d).wait_recv()
            folded = [[], []]
            for i in range(0, step, 2):
                sides = []
                for z in (c * step + i, c * step + i + 1):
                    sides.append(jnp.concatenate(
                        [r1[p, s, z].reshape(length, length) for p in range(2)], axis=0))
                done = dot(yf_ref[...], jnp.concatenate(sides, axis=1))
                for p in range(2):
                    for e in range(2):
                        part = done[p * high : (p + 1) * high, e * high : (e + 1) * high]
                        mask = mask_ref[...]
                        guest = pltpu.roll(part[hosts + extra :], length // 2, axis=1)
                        shared = part[hosts : hosts + extra] * mask + guest * (1.0 - mask)
                        folded[p].append(jnp.concatenate([part[:hosts], shared], axis=0))
            rows = step * rows_k
            at = pl.ds(pl.multiple_of(c * rows, rows), rows)
            for p in range(2):
                for m in range(size_z):
                    a2[p, s, m, at] = jnp.concatenate(
                        [part[m * rows_k : (m + 1) * rows_k] for part in folded[p]], axis=0)
            for d in order_z:
                copy2(s, c, d).start()
            rows = step * rows_k
            own = pl.ds(pl.multiple_of(c * rows, rows), rows)
            r2[:, s, pl.ds(pl.multiple_of((me_z * chunks + c) * rows, rows), rows)] = a2[:, s, me_z, own]
            return carry
        lax.fori_loop(0, chunks, forward_y, 0)

    for s in range(slots):
        def arrive2(c, carry):
            for d in range(1, size_z):
                copy2(s, c, d).wait_recv()
            return carry
        lax.fori_loop(0, chunks, arrive2, 0)

        def both_z(h, carry):
            sides = []
            for k in (2 * h, 2 * h + 1):
                sides.append(jnp.concatenate(
                    [r2[p, s, pl.ds(k, length, stride=rows_k)] for p in range(2)], axis=0))
            spectrum = dot(lf_ref[...], jnp.concatenate(sides, axis=1))
            weight = jnp.concatenate([kin_ref[2 * h], kin_ref[2 * h + 1]], axis=1)
            weight = jnp.concatenate([weight, weight], axis=0)
            done = dot(li_ref[...], spectrum * weight)
            for p in range(2):
                for e in range(2):
                    r2[p, s, pl.ds(2 * h + e, length, stride=rows_k)] = done[
                        p * high : (p + 1) * high, e * high : (e + 1) * high]
            return carry
        lax.fori_loop(0, rows_k // 2, both_z, 0)

        def leave3(c, carry):
            for d in order_z:
                copy3(s, c, d).start()
            return carry
        lax.fori_loop(0, chunks, leave3, 0)
        every = rows_z * rows_k
        r3[:, s, me_z] = r2[:, s, pl.ds(pl.multiple_of(me_z * every, every), every)]

    for s in range(slots):
        def inverse_y(c, carry):
            for d in range(1, size_z):
                copy3(s, c, d).wait_recv()
            rows = step * rows_k
            at = pl.ds(pl.multiple_of(c * rows, rows), rows)
            held = [[r3[p, s, m, at] for m in range(size_z)] for p in range(2)]
            for i in range(0, step, 2):
                sides = []
                for e in range(2):
                    both = []
                    for p in range(2):
                        part = jnp.concatenate(
                            [held[p][m][(i + e) * rows_k : (i + e + 1) * rows_k]
                             for m in range(size_z)], axis=0)
                        mask = mask_ref[...]
                        shared = part[hosts:]
                        guest = pltpu.roll(shared * (1.0 - mask), length // 2, axis=1)
                        both += [part[:hosts], shared * mask, guest]
                    sides.append(jnp.concatenate(both, axis=0))
                done = dot(yi_ref[...], jnp.concatenate(sides, axis=1))
                for p in range(2):
                    for e in range(2):
                        part = done[p * high : (p + 1) * high, e * high : (e + 1) * high]
                        r1[p, s, c * step + i + e] = part.reshape(size_y, rows_y, length)
            for d in range(1, size_y):
                copy4(s, c, d).start()
            zs = pl.ds(c * step, step)
            out_ref[:, me_y * slots + s, zs] = r1[:, s, zs, me_y]
            return carry
        lax.fori_loop(0, chunks, inverse_y, 0)

    for s in range(slots):
        def inverse_x(c, carry):
            zs = pl.ds(c * step, step)
            for d in range(size_y):
                band = (me_y + size_y - d) % size_y * slots + s
                if d > 0:
                    copy4(s, c, d).wait_recv()
                rows = jnp.concatenate(
                    [out_ref[p, band, zs].reshape(step * rows_y, length) for p in range(2)], axis=1)
                done = dot(rows, xi_ref[...])
                for p in range(2):
                    out_ref[p, band, zs] = done[:, p * high : (p + 1) * high].reshape(
                        step, rows_y, length)
            return carry
        lax.fori_loop(0, chunks, inverse_x, 0)

    for s in range(slots):
        def settle(c, carry):
            for d in range(1, size_y):
                copy1(s, c, d).wait_send()
                copy4(s, c, d).wait_send()
            for d in range(1, size_z):
                copy2(s, c, d).wait_send()
                copy3(s, c, d).wait_send()
            return carry
        lax.fori_loop(0, chunks, settle, 0)


def fused_kinetic(wavefunctions, cutoff_sq, folding, forward, inverse):
    order, mask, square = folding
    _, bands, rows_z, rows_y, length = wavefunctions.shape
    size_y, size_z = lax.axis_size("py"), lax.axis_size("pz")
    slots = bands // size_y
    rows_k = square.shape[0] // size_z
    chunks = rows_z // 4
    xf, xi = right_matrix(forward), right_matrix(inverse)
    both = np.concatenate([order, order + length])
    own_sq = lax.dynamic_slice_in_dim(jnp.asarray(square), lax.axis_index("pz") * rows_k, rows_k, 0)
    full_sq = signed_square(jnp.arange(length, dtype=jnp.int32), length)
    kinetic = weigh(own_sq[:, None, :] + full_sq[None, :, None], cutoff_sq, length)
    tables = (kinetic, xf, xi, xf.T, xi.T, xf.T[both], xi.T[:, both], jnp.asarray(mask))
    vmem = pl.BlockSpec(memory_space=pltpu.VMEM)
    near = pltpu.SemaphoreType.DMA((slots, chunks, size_y - 1))
    far = pltpu.SemaphoreType.DMA((slots, chunks, size_z - 1))
    return pl.pallas_call(
        functools.partial(main_kernel, size_y, size_z, chunks),
        out_shape=jax.ShapeDtypeStruct(wavefunctions.shape, jnp.float32),
        in_specs=[vmem] * 9,
        out_specs=vmem,
        scratch_shapes=[
            pltpu.VMEM((2, bands, rows_z, rows_y, length), jnp.float32),
            pltpu.VMEM((2, slots, rows_z, size_y, rows_y, length), jnp.float32),
            pltpu.VMEM((2, slots, size_z, rows_z * rows_k, length), jnp.float32),
            pltpu.VMEM((2, slots, length * rows_k, length), jnp.float32),
            pltpu.VMEM((2, slots, size_z, rows_z * rows_k, length), jnp.float32),
            near, near, far, far, far, far, near, near,
        ],
        compiler_params=pltpu.CompilerParams(
            collective_id=0, has_side_effects=True, vmem_limit_bytes=67043328),
    )(wavefunctions, *tables)


def gather_kernel(size_y, size_z, own_ref, out_ref, send, recv):
    me_y, me_z = lax.axis_index("py"), lax.axis_index("pz")
    me = me_y * size_z + me_z
    count = size_y * size_z
    barrier = pltpu.get_barrier_semaphore()

    def target(t):
        to = (me + t) % count
        return {"py": to // size_z, "pz": to % size_z}

    def greet(t, carry):
        pl.semaphore_signal(barrier, inc=1, device_id=target(t), device_id_type=MESH)
        return carry
    lax.fori_loop(1, count, greet, 0)
    pl.semaphore_wait(barrier, count - 1)

    def copy(t):
        return pltpu.make_async_remote_copy(
            src_ref=own_ref, dst_ref=out_ref.at[me], send_sem=send.at[t], recv_sem=recv.at[t],
            device_id=target(t), device_id_type=MESH)

    def leave(t, carry):
        copy(t).start()
        return carry
    lax.fori_loop(1, count, leave, 0)
    out_ref[me] = own_ref[...]

    def arrive(t, carry):
        copy(t).wait()
        return carry
    lax.fori_loop(1, count, arrive, 0)


def gather_sums(sums):
    size_y, size_z = lax.axis_size("py"), lax.axis_size("pz")
    count = size_y * size_z
    kinds, bands = sums.shape
    if count > 64:
        return lax.all_gather(sums, ("py", "pz"))
    own = jnp.pad(sums, ((0, 8 - kinds), (0, 128 - bands)))
    vmem = pl.BlockSpec(memory_space=pltpu.VMEM)
    every = pl.pallas_call(
        functools.partial(gather_kernel, size_y, size_z),
        out_shape=jax.ShapeDtypeStruct((count, 8, 128), jnp.float32),
        in_specs=[vmem],
        out_specs=vmem,
        scratch_shapes=[pltpu.SemaphoreType.DMA((count,)), pltpu.SemaphoreType.DMA((count,))],
        compiler_params=pltpu.CompilerParams(collective_id=1, has_side_effects=True),
    )(own)
    return every[:, :kinds, :bands]


def weigh(total, cutoff_sq, length):
    keep = (total <= cutoff_sq[0]).astype(jnp.float32)
    return 0.5 * (math.pi / length) ** 2 * total.astype(jnp.float32) * keep


def plain_kinetic(wavefunctions, kinetic, forward, inverse):
    along_x = "bzyn,kn->bzyk"
    along_y = "bznx,kn->bzkx"
    along_z = "bnyx,kn->bkyx"
    pair = (wavefunctions[0], wavefunctions[1])
    pair = transform(along_x, pair, forward)
    pair = exchange(pair, "py", 0, 2)
    pair = transform(along_y, pair, forward)
    pair = exchange(pair, "pz", 2, 1)
    pair = transform(along_z, pair, forward)
    pair = tuple(part * jnp.swapaxes(kinetic, 0, 1)[None] for part in pair)
    pair = transform(along_z, pair, inverse)
    pair = exchange(pair, "pz", 1, 2)
    pair = transform(along_y, pair, inverse)
    pair = exchange(pair, "py", 2, 0)
    pair = transform(along_x, pair, inverse)
    return jnp.stack(pair)


def body(wavefunctions, potential, cutoff_sq, locked_mask):
    length = wavefunctions.shape[4]
    forward = make_tables(length, False)
    inverse = make_tables(length, True)
    size_y, size_z = lax.axis_size("py"), lax.axis_size("pz")
    rows = length // size_z
    extra = 2 * size_z
    kept = rows - 2
    fits = extra % 8 == 0 and 4 * kept % 8 == 0 and kept > 2 and rows % 8 == 0
    fits = fits and wavefunctions.shape[2] % 4 == 0 and wavefunctions.shape[1] % size_y == 0
    folding = fold_rows(length, extra) if fits else None
    if folding is not None:
        back = fused_kinetic(wavefunctions, cutoff_sq, folding, forward, inverse)
    else:
        full_sq = signed_square(jnp.arange(length, dtype=jnp.int32), length)
        own = lax.axis_index("pz") * rows + jnp.arange(rows, dtype=jnp.int32)
        own_sq = signed_square(own, length)
        total = own_sq[:, None, None] + full_sq[None, :, None] + full_sq[None, None, :]
        kinetic = weigh(total, cutoff_sq, length)
        back = plain_kinetic(wavefunctions, kinetic, forward, inverse)
    applied = back + potential[None, None] * wavefunctions
    norm_own = jnp.sum(wavefunctions * wavefunctions, axis=(0, 2, 3, 4))
    corr_own = jnp.sum(wavefunctions * applied, axis=(0, 2, 3, 4))
    shift = jnp.where(norm_own > 0.0, corr_own / jnp.where(norm_own > 0.0, norm_own, 1.0), 0.0)
    rest = applied - shift[None, :, None, None, None] * wavefunctions
    rest_sq = jnp.sum(rest * rest, axis=(0, 2, 3, 4))
    rest_dot = jnp.sum(rest * wavefunctions, axis=(0, 2, 3, 4))
    sums = jnp.stack([norm_own, corr_own, shift, rest_sq, rest_dot])
    every = gather_sums(sums)
    norm_all, corr_all, shift_all, sq_all, dot_all = (every[:, i] for i in range(5))
    norm_sq = jnp.sum(norm_all, axis=0)
    rayleigh = jnp.sum(corr_all, axis=0) / norm_sq
    gap = shift_all - rayleigh[None]
    residual_sq = jnp.sum(sq_all + 2.0 * gap * dot_all + gap * gap * norm_all, axis=0)
    residual_sq = jnp.maximum(residual_sq, 0.0)
    residual_norm = jnp.sqrt(residual_sq / norm_sq) * (1.0 - locked_mask.astype(jnp.float32))
    return (applied, rayleigh, residual_norm)


def solution(mesh):
    in_specs = (P(None, None, "pz", "py", None), P("pz", "py", None), P(), P())
    out_specs = (P(None, None, "pz", "py", None), P(), P())
    return jax.shard_map(body, mesh=mesh, in_specs=in_specs, out_specs=out_specs, check_vma=False)
```
